8 devices in a mesh: dp: 2 (over y, z), sp: 4 (over x, core).
Axes of the slice: x: 2, y: 2, z: 1, core: 2. Of those that a mesh axis runs over, the one named last changes fastest.
Arguments:
- x: bfloat16 [8192, 2048], P(('dp', 'sp')), parts along dimension 0
- gain: bfloat16 [2048], replicated
- wq: bfloat16 [2048, 2048], P('sp')
- wk: bfloat16 [2048, 2048], P('sp')
- wv: bfloat16 [2048, 2048], P('sp')
- wo: bfloat16 [2048, 2048], P('sp')
Outputs:
- output: bfloat16 [8192, 2048], P(('dp', 'sp')), parts along dimension 0
There are 2 independent parts. The reference program is written for one: setup_inputs(seed, part) draws one part's arguments, and reference() takes and returns one part's arrays. A program takes and returns all parts, laid end to end along the dimension named above; an argument that names none is the same for every part.
All inputs are finite; a program needn't handle non-finite values.
Results may differ from the reference program's by a relative error of at most 0.012.
Values are sent between devices in bfloat16 or wider.
A program may use at most 2 GiB of HBM per device.

```python
import jax
import jax.numpy as jnp
from jax import lax

ROWS = 4096
D = 2048
HEADS = 16
KV_HEADS = 16
HEAD = 128
THETA = 10000


def setup_inputs(seed: int = 0, part: int = 0) -> dict:
    kx, kn, kq, kk, kv, ko = jax.random.split(jax.random.key(seed), 6)

    def weights(key, rows, columns):
        return jax.random.normal(key, (rows, columns), jnp.float32) * rows**-0.5

    drawn = {
        "x": jax.random.normal(jax.random.fold_in(kx, part), (ROWS, D), jnp.float32),
        "gain": 1 + 0.1 * jax.random.normal(kn, (D,), jnp.float32),
        "wq": 2 * weights(kq, D, HEADS * HEAD),
        "wk": 2 * weights(kk, D, KV_HEADS * HEAD),
        "wv": 4 * weights(kv, D, KV_HEADS * HEAD),
        "wo": weights(ko, HEADS * HEAD, D),
    }
    return {k: v.astype(jnp.bfloat16) for k, v in drawn.items()}


def normed(x, gain):
    wide = x.astype(jnp.float32)
    scale = lax.rsqrt(jnp.mean(wide * wide, -1, keepdims=True) + 1e-6)
    return (wide * scale * gain.astype(jnp.float32)).astype(jnp.bfloat16)


def turned(t, place, theta):
    half = t.shape[-1] // 2
    angle = place.astype(jnp.float32)[:, None] * theta ** (-jnp.arange(half, dtype=jnp.float32) / half)
    cos, sin = jnp.cos(angle)[:, None], jnp.sin(angle)[:, None]
    a, b = t[..., :half].astype(jnp.float32), t[..., half:].astype(jnp.float32)
    return jnp.concatenate([a * cos - b * sin, b * cos + a * sin], -1).astype(jnp.bfloat16)


def matmul(a, w):
    return jnp.dot(a, w, preferred_element_type=jnp.float32).astype(jnp.bfloat16)


def einsum(form, a, b):
    return jnp.einsum(form, a.astype(jnp.float32), b.astype(jnp.float32))


def attention(q, k, v):
    scores = einsum("tgsd,ugd->gstu", q, k) * q.shape[-1] ** -0.5
    token = jnp.arange(q.shape[0])
    scores = jnp.where(token[:, None] >= token, scores, -jnp.inf)
    weights = jax.nn.softmax(scores, -1).astype(jnp.bfloat16)
    return einsum("gstu,ugd->tgsd", weights, v).astype(jnp.bfloat16)


def reference(x, gain, wq, wk, wv, wo):
    a, place = normed(x, gain), jnp.arange(ROWS)
    q = turned(matmul(a, wq).reshape(ROWS, HEADS, HEAD), place, THETA).reshape(ROWS, KV_HEADS, -1, HEAD)
    k = turned(matmul(a, wk).reshape(ROWS, KV_HEADS, HEAD), place, THETA)
    v = matmul(a, wv).reshape(ROWS, KV_HEADS, HEAD)
    seen = attention(q, k, v).reshape(ROWS, HEADS * HEAD)
    return (x.astype(jnp.float32) + jnp.dot(seen, wo, preferred_element_type=jnp.float32)).astype(jnp.bfloat16)
```

```python
import functools

import numpy as np

import jax
import jax.numpy as jnp
from jax import lax
from jax.experimental import pallas as pl
from jax.experimental.pallas import tpu as pltpu
from jax.sharding import PartitionSpec as P

MESH = pl.DeviceIdType.MESH
HEAD = 128
THETA = 10000
NEG = -1e30
HIDDEN = 2 * NEG
LOG2E = 1.4426950408889634
DEVICES = 4
OWN = 1024
ROWS = DEVICES * OWN
D = 2048
HEADS = 4
WIDE = HEADS * HEAD
PIECE = 256
CHUNK = 512
SUMS = 16


def _dot(a, b, ca, cb):
    return lax.dot_general(a, b, (((ca,), (cb,)), ((), ())), preferred_element_type=jnp.float32)


def _rows(i, size):
    return pl.ds(pl.multiple_of(i * size, size), size)


def _kernel(x_ref, gain_ref, wq_ref, wk_ref, wv_ref, wo_ref, near_ref, far_ref, y_ref,
            a_s, w_s, wo_s, q_s, k_s, v_s, out_s, seen_s, top_s, mix_s,
            load_sem, wx_s, wx_r, wy_s, wy_r, wp_s, wp_r, ap_s, ap_r, ax_s, ax_r, af_s, af_r,
            op_s, op_r, ox_s, ox_r, oy_s, oy_r, of_s, of_r, s_s, s_r, store_sem):
    g, me = lax.axis_index("dp"), lax.axis_index("sp")
    chip, core = me // 2, me % 2
    far = (1 - chip) * 2
    partner, cross = chip * 2 + 1 - core, far + core
    turned_core = core + g - 2 * core * g
    wx = far + turned_core
    wx_other = far + 1 - turned_core
    peer = (1 - g, me)
    weights = (wq_ref, wk_ref, wv_ref)

    def remote(src, dst, send, recv, to):
        return pltpu.make_async_remote_copy(src, dst, send, recv, device_id=to, device_id_type=MESH)

    barrier = pltpu.get_barrier_semaphore()
    for to in ((g, partner), (g, cross), (g, far + 1 - core), peer):
        pl.semaphore_signal(barrier, inc=1, device_id=to, device_id_type=MESH)
    pl.semaphore_wait(barrier, 4)

    def w_cross(n, to, rows_of):
        m, half = n // 2, n % 2
        return remote(weights[m].at[pl.ds(half * 256, 256), _rows(to, WIDE)],
                      w_s.at[m, pl.ds(pl.multiple_of(rows_of * 512 + half * 256, 256), 256)], wx_s.at[n], wx_r.at[n], (g, to))

    def w_trade(n, rows_of):
        m, half = n // 2, n % 2
        at = w_s.at[m, pl.ds(pl.multiple_of(rows_of * 512 + half * 256, 256), 256)]
        return remote(at, at, wy_s.at[n], wy_r.at[n], peer)

    def w_partner(m, rows_of):
        return remote(weights[m].at[:, _rows(partner, WIDE)], w_s.at[m, _rows(rows_of, 512)], wp_s.at[m], wp_r.at[m], (g, partner))

    def a_piece(n, send, recv, to):
        at = a_s.at[_rows(n, PIECE)]
        return remote(at, at, send, recv, to)

    def wo_part(rows_of, part):
        return wo_s.at[pl.ds(pl.multiple_of(rows_of * 512 + part * 256, 256), 256)]

    def wo_cross(rows_of):
        return remote(wo_ref.at[_rows(g, 256)], wo_part(rows_of, g), ox_s, ox_r, (g, cross))

    def wo_trade(part):
        at = wo_part(cross, part)
        return remote(at, at, oy_s, oy_r, peer)

    def wo_forward(rows_of, part, n):
        at = wo_part(rows_of, part)
        return remote(at, at, of_s.at[n], of_r.at[n], (g, partner))

    def wo_partner(rows_of):
        return remote(wo_ref, wo_s.at[_rows(rows_of, 512)], op_s, op_r, (g, partner))

    def result(n, source, to):
        return remote(out_s.at[_rows(n, PIECE)], seen_s.at[_rows(n % 4, PIECE), _rows(source, WIDE)], s_s.at[n], s_r.at[source, n % 4], (g, to))

    load_x = [pltpu.make_async_copy(x_ref.at[pl.ds(n * PIECE, PIECE)], a_s.at[_rows(me * 4 + n, PIECE)], load_sem.at[n]) for n in range(4)]
    load_w = [pltpu.make_async_copy(weights[m].at[:, _rows(me, WIDE)], w_s.at[m, _rows(me, 512)], load_sem.at[4 + m]) for m in range(3)]
    load_wo = pltpu.make_async_copy(wo_ref, wo_s.at[_rows(me, 512)], load_sem.at[7])
    again_x = [pltpu.make_async_copy(x_ref.at[pl.ds(n * PIECE, PIECE)], a_s.at[_rows(me * 4 + n, PIECE)], load_sem.at[8 + n]) for n in range(4)]

    def store(n):
        return pltpu.make_async_copy(a_s.at[_rows(me * 4 + n, PIECE)], y_ref.at[_rows(n, PIECE)], store_sem.at[n])

    for n in range(6):
        w_cross(n, wx, me).start()
    for copy in load_x:
        copy.start()
    for m in range(3):
        w_partner(m, me).start()
    for copy in load_w:
        copy.start()

    for n in range(4):
        load_x[n].wait()
        mine = _rows(me * 4 + n, PIECE)
        wide = a_s[mine, :].astype(jnp.float32)
        scale = lax.rsqrt(jnp.mean(wide * wide, -1, keepdims=True) + 1e-6)
        a_s[mine, :] = (wide * scale * gain_ref[...].astype(jnp.float32)).astype(jnp.bfloat16)
        a_piece(me * 4 + n, ap_s.at[n], ap_r.at[n], (g, partner)).start()
    for n in range(4):
        a_piece(partner * 4 + n, ap_s.at[n], ap_r.at[n], (g, partner)).wait_recv()
    for r in range(4):
        a_piece(chip * 8 + 2 * r + core, ax_s.at[r], ax_r.at[r], (g, cross)).start()
    wo_cross(me).start()
    wo_partner(me).start()
    load_wo.start()

    for n in range(6):
        w_cross(n, me, wx).wait_recv()
        w_trade(n, wx).start()
    for copy in load_w:
        copy.wait()
    for m in range(3):
        w_partner(m, partner).wait_recv()
    for n in range(6):
        w_trade(n, wx_other).wait_recv()

    v_s[:, HEAD:, :] = jnp.ones((HEADS, SUMS, ROWS), jnp.bfloat16)

    def project(n):
        rows = _rows(n, CHUNK)
        cos, sin = [], []
        for s in range(2):
            near_cos, near_sin = near_ref[0], near_ref[1]
            far_cos, far_sin = far_ref[0, pl.ds(2 * n + s, 1), :], far_ref[1, pl.ds(2 * n + s, 1), :]
            cos.append(far_cos * near_cos - far_sin * near_sin)
            sin.append(far_sin * near_cos + far_cos * near_sin)
        cos, sin = jnp.concatenate(cos, 0), jnp.concatenate(sin, 0)
        for m, to in ((0, q_s), (1, k_s)):
            got = _dot(a_s[rows, :], w_s[m], 1, 0).astype(jnp.bfloat16).astype(jnp.float32)
            for h in range(HEADS):
                t = got[:, h * HEAD : (h + 1) * HEAD]
                to[h, rows, :] = (t * cos + pltpu.roll(t, HEAD // 2, 1) * sin).astype(jnp.bfloat16)
        got = _dot(a_s[rows, :], w_s[2], 1, 0)
        for h in range(HEADS):
            v_s[h, :HEAD, rows] = got[:, h * HEAD : (h + 1) * HEAD].T.astype(jnp.bfloat16)

    e = HEAD**-0.5 * LOG2E

    def attend(n):
        top_s[...] = jnp.full(top_s.shape, NEG, jnp.float32)
        mix_s[...] = jnp.zeros(mix_s.shape, jnp.float32)
        queries = _rows(n, CHUNK)

        def block(j, masked):
            keys = _rows(j, CHUNK)
            scores = [_dot(k_s[h, keys, :], q_s[h, queries, :], 1, 1) for h in range(HEADS)]
            if masked:
                ok = lax.broadcasted_iota(jnp.int32, (CHUNK, CHUNK), 1) >= lax.broadcasted_iota(jnp.int32, (CHUNK, CHUNK), 0)
            weights, keeps = [], []
            for h, s in enumerate(scores):
                if masked:
                    s = jnp.where(ok, s, HIDDEN)
                old = top_s[h : h + 1, :]
                top = jnp.maximum(old, s.max(axis=0, keepdims=True))
                top_s[h : h + 1, :] = top
                weights.append(jnp.exp2((s - top) * e).astype(jnp.bfloat16))
                keeps.append(jnp.exp2((old - top) * e))
            for h in range(HEADS):
                mix_s[h] = mix_s[h] * keeps[h] + _dot(v_s[h, :, keys], weights[h], 1, 0)

        lax.fori_loop(0, n, lambda j, _: block(j, False), None)
        block(n, True)
        for h in range(HEADS):
            total = mix_s[h, HEAD : HEAD + 1, :]
            out_s[queries, h * HEAD : (h + 1) * HEAD] = (mix_s[h, :HEAD, :] * (1 / total)).T.astype(jnp.bfloat16)

    def pass_wo_on():
        wo_cross(cross).wait_recv()
        wo_trade(g).start()
        wo_forward(cross, g, 0).start()

    lax.fori_loop(0, 4, lambda r, _: project(chip * 4 + r), None)

    def step(n, _):
        r, owner = n % 4, n // 2

        @pl.when(n // 4 != chip)
        def _():
            mine = far * 4 + 2 * r + core
            a_piece(mine, ax_s.at[r], ax_r.at[r], (g, cross)).wait_recv()
            a_piece(mine, af_s.at[r], af_r.at[r], (g, partner)).start()
            a_piece(far * 4 + 2 * r + 1 - core, af_s.at[r], af_r.at[r], (g, partner)).wait_recv()
            project(n)

        @pl.when((n == 6) & (chip == 1))
        def _():
            pass_wo_on()

        attend(n)

        @pl.when(owner == me)
        def _():
            seen_s[_rows(n % 2, CHUNK), _rows(me, WIDE)] = out_s[_rows(n, CHUNK), :]

        @pl.when(owner != me)
        def _():
            result(2 * n, me, owner).start()
            result(2 * n + 1, me, owner).start()

    lax.fori_loop(0, 8, step, None)

    for r in range(4):
        a_piece(me * 4 + r, ap_s.at[r], ap_r.at[r], (g, partner)).wait_send()
        a_piece(chip * 8 + 2 * r + core, ax_s.at[r], ax_r.at[r], (g, cross)).wait_send()
    for copy in again_x:
        copy.start()

    @pl.when(chip == 0)
    def _():
        pass_wo_on()

    wo_trade(1 - g).wait_recv()
    wo_forward(cross, 1 - g, 1).start()
    load_wo.wait()
    wo_partner(partner).wait_recv()
    for n in range(2):
        part = g if n == 0 else 1 - g
        wo_forward(far + 1 - core, part, n).wait_recv()
    for copy in again_x:
        copy.wait()

    def last(n, _):
        for other in (partner, cross, far + 1 - core):
            result(me * 4 + n, other, me).wait_recv()
        mine = _rows(me * 4 + n, PIECE)

        def columns(j, _):
            at = _rows(j, 512)
            y = _dot(seen_s[_rows(n, PIECE), :], wo_s[:, at], 1, 0)
            a_s[mine, at] = (a_s[mine, at].astype(jnp.float32) + y).astype(jnp.bfloat16)

        lax.fori_loop(0, 4, columns, None)
        store(n).start()

    lax.fori_loop(0, 4, last, None)

    for n in range(6):
        w_cross(n, wx, me).wait_send()
        w_trade(n, wx).wait_send()
    for m in range(3):
        w_partner(m, me).wait_send()
    for r in range(4):
        a_piece(far * 4 + 2 * r + core, af_s.at[r], af_r.at[r], (g, partner)).wait_send()
    wo_cross(me).wait_send()
    wo_partner(me).wait_send()
    wo_trade(g).wait_send()
    wo_forward(cross, g, 0).wait_send()
    wo_forward(cross, 1 - g, 1).wait_send()

    def sent(n, _):
        @pl.when(n // 4 != me)
        def _():
            result(n, me, n // 4).wait_send()

    lax.fori_loop(0, 16, sent, None)
    for n in range(4):
        store(n).wait()


def _turns(places):
    half = HEAD // 2
    angle = places[:, None].astype(np.float64) * THETA ** (-np.arange(half) / half)
    cos, sin = np.cos(angle), np.sin(angle)
    return np.stack([np.concatenate([cos, cos], 1), np.concatenate([-sin, sin], 1)]).astype(np.float32)


def solution(mesh):
    def step(x, gain, wq, wk, wv, wo):
        vmem, any_ = pl.BlockSpec(memory_space=pltpu.VMEM), pl.BlockSpec(memory_space=pl.ANY)
        bf16, dma = jnp.bfloat16, pltpu.SemaphoreType.DMA
        return pl.pallas_call(
            _kernel,
            out_shape=jax.ShapeDtypeStruct((OWN, D), bf16),
            in_specs=[any_, vmem, any_, any_, any_, any_, vmem, vmem],
            out_specs=any_,
            scratch_shapes=[
                pltpu.VMEM((ROWS, D), bf16),
                pltpu.VMEM((3, D, WIDE), bf16),
                pltpu.VMEM((D, D), bf16),
                pltpu.VMEM((HEADS, ROWS, HEAD), bf16),
                pltpu.VMEM((HEADS, ROWS, HEAD), bf16),
                pltpu.VMEM((HEADS, HEAD + SUMS, ROWS), bf16),
                pltpu.VMEM((ROWS, WIDE), bf16),
                pltpu.VMEM((OWN, D), bf16),
                pltpu.VMEM((HEADS, CHUNK), jnp.float32),
                pltpu.VMEM((HEADS, HEAD + SUMS, CHUNK), jnp.float32),
                dma((12,)),
                dma((6,)), dma((6,)), dma((6,)), dma((6,)), dma((3,)), dma((3,)),
                dma((4,)), dma((4,)), dma((4,)), dma((4,)), dma((4,)), dma((4,)),
                dma, dma, dma, dma, dma, dma, dma((2,)), dma((2,)),
                dma((16,)), dma((4, 4)), dma((4,)),
            ],
            compiler_params=pltpu.CompilerParams(collective_id=0, has_side_effects=True, vmem_limit_bytes=67043328),
        )(x, gain.reshape(1, D), wq, wk, wv, wo, jnp.asarray(_turns(np.arange(PIECE))), jnp.asarray(_turns(np.arange(ROWS // PIECE) * PIECE)))

    tokens, whole = P(("dp", "sp"), None), P("sp", None)
    return jax.shard_map(
        step,
        mesh=mesh,
        in_specs=(tokens, P(None), whole, whole, whole, whole),
        out_specs=tokens,
        check_vma=False,
    )
```

```python
import functools

import numpy as np

import jax
import jax.numpy as jnp
from jax import lax
from jax.experimental import pallas as pl
from jax.experimental.pallas import tpu as pltpu
from jax.sharding import PartitionSpec as P

MESH = pl.DeviceIdType.MESH
HEAD = 128
THETA = 10000
NEG = -1e30
HIDDEN = 2 * NEG
LOG2E = 1.4426950408889634
DEVICES = 4
OWN = 1024
ROWS = DEVICES * OWN
D = 2048
HEADS = 4
WIDE = HEADS * HEAD
PIECE = 256
TILE = 512
CHUNK = 512
SUMS = 16


def _dot(a, b, ca, cb):
    return lax.dot_general(a, b, (((ca,), (cb,)), ((), ())), preferred_element_type=jnp.float32)


def _rows(i, size):
    return pl.ds(pl.multiple_of(i * size, size), size)


def _kernel(x_ref, gain_ref, wq_ref, wk_ref, wv_ref, wo_ref, near_ref, far_ref, y_ref,
            a_s, w_s, wo_s, q_s, k_s, v_s, out_s, seen_s, part_s, top_s, mix_s,
            load_sem, wx_s, wx_r, wy_s, wy_r, wp_s, wp_r, ap_s, ap_r, ax_s, ax_r, af_s, af_r,
            op_s, op_r, ox_s, ox_r, oy_s, oy_r, of_s, of_r, s_s, s_r, store_sem):
    g, me = lax.axis_index("dp"), lax.axis_index("sp")
    chip, core = me // 2, me % 2
    far = (1 - chip) * 2
    partner, cross = chip * 2 + 1 - core, far + core
    turned_core = core + g - 2 * core * g
    wx = far + turned_core
    wx_other = far + 1 - turned_core
    peer = (1 - g, me)
    weights = (wq_ref, wk_ref, wv_ref)

    def remote(src, dst, send, recv, to):
        return pltpu.make_async_remote_copy(src, dst, send, recv, device_id=to, device_id_type=MESH)

    barrier = pltpu.get_barrier_semaphore()
    for to in ((g, partner), (g, cross), (g, far + 1 - core), peer):
        pl.semaphore_signal(barrier, inc=1, device_id=to, device_id_type=MESH)
    pl.semaphore_wait(barrier, 4)

    def away(owner):
        return (owner - me + 3) % 4 % 3

    def w_cross(n, to, rows_of):
        m, half = n // 2, n % 2
        return remote(weights[m].at[pl.ds(half * 256, 256), _rows(to, WIDE)],
                      w_s.at[m, pl.ds(pl.multiple_of(rows_of * 512 + half * 256, 256), 256)], wx_s.at[n], wx_r.at[n], (g, to))

    def w_trade(n, rows_of):
        m, half = n // 2, n % 2
        at = w_s.at[m, pl.ds(pl.multiple_of(rows_of * 512 + half * 256, 256), 256)]
        return remote(at, at, wy_s.at[n], wy_r.at[n], peer)

    def w_partner(m, rows_of):
        return remote(weights[m].at[:, _rows(partner, WIDE)], w_s.at[m, _rows(rows_of, 512)], wp_s.at[m], wp_r.at[m], (g, partner))

    def a_piece(n, send, recv, to):
        at = a_s.at[_rows(n, PIECE)]
        return remote(at, at, send, recv, to)

    def wo_part(rows_of, part):
        return wo_s.at[pl.ds(pl.multiple_of(rows_of * 512 + part * 256, 256), 256)]

    def wo_cross(rows_of):
        return remote(wo_ref.at[_rows(g, 256)], wo_part(rows_of, g), ox_s, ox_r, (g, cross))

    def wo_trade(part):
        at = wo_part(cross, part)
        return remote(at, at, oy_s, oy_r, peer)

    def wo_forward(rows_of, part, n):
        at = wo_part(rows_of, part)
        return remote(at, at, of_s.at[n], of_r.at[n], (g, partner))

    def wo_partner(rows_of):
        return remote(wo_ref, wo_s.at[_rows(rows_of, 512)], op_s, op_r, (g, partner))

    def result(n, source, to):
        return remote(out_s.at[_rows(away(n // 4) * 4 + n % 4, PIECE)], seen_s.at[_rows(n % 4, PIECE), _rows(source, WIDE)], s_s.at[n], s_r.at[source, n % 4], (g, to))

    load_x = [pltpu.make_async_copy(x_ref.at[pl.ds(n * PIECE, PIECE)], a_s.at[_rows(me * 4 + n, PIECE)], load_sem.at[n]) for n in range(4)]
    load_w = [pltpu.make_async_copy(weights[m].at[:, _rows(me, WIDE)], w_s.at[m, _rows(me, 512)], load_sem.at[4 + m]) for m in range(3)]
    load_wo = pltpu.make_async_copy(wo_ref, wo_s.at[_rows(me, 512)], load_sem.at[7])
    again_x = [pltpu.make_async_copy(x_ref.at[pl.ds(n * PIECE, PIECE)], a_s.at[_rows(me * 4 + n, PIECE)], load_sem.at[8 + n]) for n in range(4)]

    def store(n, j):
        at = _rows(j, TILE)
        return pltpu.make_async_copy(a_s.at[_rows(me * 4 + n, PIECE), at], y_ref.at[_rows(n, PIECE), at], store_sem.at[n, j])

    for n in range(6):
        w_cross(n, wx, me).start()
    for copy in load_x:
        copy.start()
    for m in range(3):
        w_partner(m, me).start()
    for copy in load_w:
        copy.start()

    for n in range(4):
        load_x[n].wait()
        mine = _rows(me * 4 + n, PIECE)
        wide = a_s[mine, :].astype(jnp.float32)
        scale = lax.rsqrt(jnp.mean(wide * wide, -1, keepdims=True) + 1e-6)
        a_s[mine, :] = (wide * scale * gain_ref[...].astype(jnp.float32)).astype(jnp.bfloat16)
        a_piece(me * 4 + n, ap_s.at[n], ap_r.at[n], (g, partner)).start()
    for n in range(4):
        a_piece(partner * 4 + n, ap_s.at[n], ap_r.at[n], (g, partner)).wait_recv()
    for r in range(4):
        a_piece(chip * 8 + 2 * r + core, ax_s.at[r], ax_r.at[r], (g, cross)).start()
    wo_cross(me).start()
    wo_partner(me).start()
    load_wo.start()

    for n in range(6):
        w_cross(n, me, wx).wait_recv()
        w_trade(n, wx).start()
    for copy in load_w:
        copy.wait()
    for m in range(3):
        w_partner(m, partner).wait_recv()
    for n in range(6):
        w_trade(n, wx_other).wait_recv()

    v_s[:, HEAD:, :] = jnp.ones((HEADS, SUMS, ROWS), jnp.bfloat16)

    def q_rows(n):
        return _rows(jnp.where(n // 4 == chip, n % 4, 4), CHUNK)

    def project(n):
        rows = _rows(n, CHUNK)
        cos, sin = [], []
        for s in range(2):
            near_cos, near_sin = near_ref[0], near_ref[1]
            far_cos, far_sin = far_ref[0, pl.ds(2 * n + s, 1), :], far_ref[1, pl.ds(2 * n + s, 1), :]
            cos.append(far_cos * near_cos - far_sin * near_sin)
            sin.append(far_sin * near_cos + far_cos * near_sin)
        cos, sin = jnp.concatenate(cos, 0), jnp.concatenate(sin, 0)
        for m, to in ((0, q_s), (1, k_s)):
            got = _dot(a_s[rows, :], w_s[m], 1, 0).astype(jnp.bfloat16).astype(jnp.float32)
            for h in range(HEADS):
                t = got[:, h * HEAD : (h + 1) * HEAD]
                to[h, q_rows(n) if m == 0 else rows, :] = (t * cos + pltpu.roll(t, HEAD // 2, 1) * sin).astype(jnp.bfloat16)
        got = _dot(a_s[rows, :], w_s[2], 1, 0)
        for h in range(HEADS):
            v_s[h, :HEAD, rows] = got[:, h * HEAD : (h + 1) * HEAD].T.astype(jnp.bfloat16)

    e = HEAD**-0.5 * LOG2E

    def attend(n):
        top_s[...] = jnp.full(top_s.shape, NEG, jnp.float32)
        mix_s[...] = jnp.zeros(mix_s.shape, jnp.float32)
        def block(j, masked):
            keys = _rows(j, CHUNK)
            scores = [_dot(k_s[h, keys, :], q_s[h, q_rows(n), :], 1, 1) for h in range(HEADS)]
            if masked:
                ok = lax.broadcasted_iota(jnp.int32, (CHUNK, CHUNK), 1) >= lax.broadcasted_iota(jnp.int32, (CHUNK, CHUNK), 0)
            weights, keeps = [], []
            for h, s in enumerate(scores):
                if masked:
                    s = jnp.where(ok, s, HIDDEN)
                old = top_s[h : h + 1, :]
                top = jnp.maximum(old, s.max(axis=0, keepdims=True))
                top_s[h : h + 1, :] = top
                weights.append(jnp.exp2((s - top) * e).astype(jnp.bfloat16))
                keeps.append(jnp.exp2((old - top) * e))
            for h in range(HEADS):
                mix_s[h] = mix_s[h] * keeps[h] + _dot(v_s[h, :, keys], weights[h], 1, 0)

        lax.fori_loop(0, n, lambda j, _: block(j, False), None)
        block(n, True)

    def results():
        each = []
        for h in range(HEADS):
            total = mix_s[h, HEAD : HEAD + 1, :]
            each.append((mix_s[h, :HEAD, :] * (1 / total)).T.astype(jnp.bfloat16))
        return jnp.concatenate(each, axis=1)

    def pass_wo_on():
        wo_cross(cross).wait_recv()
        wo_trade(g).start()
        wo_forward(cross, g, 0).start()

    lax.fori_loop(0, 4, lambda r, _: project(chip * 4 + r), None)

    def step(n, _):
        r, owner = n % 4, n // 2

        @pl.when(n // 4 != chip)
        def _():
            mine = far * 4 + 2 * r + core
            a_piece(mine, ax_s.at[r], ax_r.at[r], (g, cross)).wait_recv()
            a_piece(mine, af_s.at[r], af_r.at[r], (g, partner)).start()
            a_piece(far * 4 + 2 * r + 1 - core, af_s.at[r], af_r.at[r], (g, partner)).wait_recv()
            project(n)

        @pl.when((n == 6) & (chip == 1))
        def _():
            pass_wo_on()

        attend(n)

        @pl.when(owner == me)
        def _():
            seen_s[_rows(n % 2, CHUNK), _rows(me, WIDE)] = results()

        @pl.when(owner != me)
        def _():
            out_s[_rows(away(owner) * 2 + n % 2, CHUNK), :] = results()
            result(2 * n, me, owner).start()
            result(2 * n + 1, me, owner).start()

    lax.fori_loop(0, 8, step, None)

    for r in range(4):
        a_piece(me * 4 + r, ap_s.at[r], ap_r.at[r], (g, partner)).wait_send()
        a_piece(chip * 8 + 2 * r + core, ax_s.at[r], ax_r.at[r], (g, cross)).wait_send()
    for copy in again_x:
        copy.start()

    @pl.when(chip == 0)
    def _():
        pass_wo_on()

    wo_trade(1 - g).wait_recv()
    wo_forward(cross, 1 - g, 1).start()
    load_wo.wait()
    wo_partner(partner).wait_recv()
    for n in range(2):
        part = g if n == 0 else 1 - g
        wo_forward(far + 1 - core, part, n).wait_recv()
    for copy in again_x:
        copy.wait()

    def arrive(n, *others):
        for other in others:
            result(me * 4 + n, other, me).wait_recv()

    def product(n, j, start, depth):
        part = pl.ds(pl.multiple_of(start, OWN), depth)
        return _dot(seen_s[_rows(n, PIECE), part], wo_s[part, _rows(j, TILE)], 1, 0)

    def put(n, j, y):
        mine, at = _rows(me * 4 + n, PIECE), _rows(j, TILE)
        a_s[mine, at] = (a_s[mine, at].astype(jnp.float32) + y).astype(jnp.bfloat16)
        store(n, j).start()

    def whole(n, _):
        arrive(n, partner, cross, far + 1 - core)
        lax.fori_loop(0, D // TILE, lambda j, _: put(n, j, product(n, j, 0, D)), None)

    lax.fori_loop(0, 3, whole, None)

    arrive(3, partner)

    def near(j, _):
        part_s[:, _rows(j, TILE)] = product(3, j, chip * OWN, OWN)

    lax.fori_loop(0, D // TILE, near, None)
    arrive(3, cross, far + 1 - core)
    lax.fori_loop(0, D // TILE, lambda j, _: put(3, j, part_s[:, _rows(j, TILE)] + product(3, j, far * WIDE, OWN)), None)

    for n in range(6):
        w_cross(n, wx, me).wait_send()
        w_trade(n, wx).wait_send()
    for m in range(3):
        w_partner(m, me).wait_send()
    for r in range(4):
        a_piece(far * 4 + 2 * r + core, af_s.at[r], af_r.at[r], (g, partner)).wait_send()
    wo_cross(me).wait_send()
    wo_partner(me).wait_send()
    wo_trade(g).wait_send()
    wo_forward(cross, g, 0).wait_send()
    wo_forward(cross, 1 - g, 1).wait_send()

    def sent(n, _):
        @pl.when(n // 4 != me)
        def _():
            result(n, me, n // 4).wait_send()

    lax.fori_loop(0, 16, sent, None)
    for n in range(4):
        for j in range(D // TILE):
            store(n, j).wait()


def _turns(places):
    half = HEAD // 2
    angle = places[:, None].astype(np.float64) * THETA ** (-np.arange(half) / half)
    cos, sin = np.cos(angle), np.sin(angle)
    return np.stack([np.concatenate([cos, cos], 1), np.concatenate([-sin, sin], 1)]).astype(np.float32)


def solution(mesh):
    def step(x, gain, wq, wk, wv, wo):
        vmem, any_ = pl.BlockSpec(memory_space=pltpu.VMEM), pl.BlockSpec(memory_space=pl.ANY)
        bf16, dma = jnp.bfloat16, pltpu.SemaphoreType.DMA
        return pl.pallas_call(
            _kernel,
            out_shape=jax.ShapeDtypeStruct((OWN, D), bf16),
            in_specs=[any_, vmem, any_, any_, any_, any_, vmem, vmem],
            out_specs=any_,
            scratch_shapes=[
                pltpu.VMEM((ROWS, D), bf16),
                pltpu.VMEM((3, D, WIDE), bf16),
                pltpu.VMEM((D, D), bf16),
                pltpu.VMEM((HEADS, 5 * CHUNK, HEAD), bf16),
                pltpu.VMEM((HEADS, ROWS, HEAD), bf16),
                pltpu.VMEM((HEADS, HEAD + SUMS, ROWS), bf16),
                pltpu.VMEM((ROWS - OWN, WIDE), bf16),
                pltpu.VMEM((OWN, D), bf16),
                pltpu.VMEM((PIECE, D), jnp.float32),
                pltpu.VMEM((HEADS, CHUNK), jnp.float32),
                pltpu.VMEM((HEADS, HEAD + SUMS, CHUNK), jnp.float32),
                dma((12,)),
                dma((6,)), dma((6,)), dma((6,)), dma((6,)), dma((3,)), dma((3,)),
                dma((4,)), dma((4,)), dma((4,)), dma((4,)), dma((4,)), dma((4,)),
                dma, dma, dma, dma, dma, dma, dma((2,)), dma((2,)),
                dma((16,)), dma((4, 4)), dma((4, D // TILE)),
            ],
            compiler_params=pltpu.CompilerParams(collective_id=0, has_side_effects=True, vmem_limit_bytes=67043328),
        )(x, gain.reshape(1, D), wq, wk, wv, wo, jnp.asarray(_turns(np.arange(PIECE))), jnp.asarray(_turns(np.arange(ROWS // PIECE) * PIECE)))

    tokens, whole = P(("dp", "sp"), None), P("sp", None)
    return jax.shard_map(
        step,
        mesh=mesh,
        in_specs=(tokens, P(None), whole, whole, whole, whole),
        out_specs=tokens,
        check_vma=False,
    )
```

```python
import functools

import numpy as np

import jax
import jax.numpy as jnp
from jax import lax
from jax.experimental import pallas as pl
from jax.experimental.pallas import tpu as pltpu
from jax.sharding import PartitionSpec as P

MESH = pl.DeviceIdType.MESH
HEAD = 128
THETA = 10000
NEG = -1e30
HIDDEN = 2 * NEG
LOG2E = 1.4426950408889634
DEVICES = 4
OWN = 1024
ROWS = DEVICES * OWN
D = 2048
HEADS = 4
WIDE = HEADS * HEAD
PIECE = 256
TILE = 512
CHUNK = 512
SUMS = 16


def _dot(a, b, ca, cb):
    return lax.dot_general(a, b, (((ca,), (cb,)), ((), ())), preferred_element_type=jnp.float32)


def _rows(i, size):
    return pl.ds(pl.multiple_of(i * size, size), size)


def _kernel(x_ref, gain_hbm, wq_ref, wk_ref, wv_ref, wo_ref, near_hbm, far_hbm, y_ref, gain_ref, near_ref, far_ref,
            a_s, w_s, wo_s, q_s, k_s, v_s, out_s, seen_s, part_s, top_s, mix_s,
            load_sem, wx_s, wx_r, wy_s, wy_r, wp_s, wp_r, ap_s, ap_r, ax_s, ax_r, af_s, af_r,
            op_s, op_r, ox_s, ox_r, oy_s, oy_r, of_s, of_r, s_s, s_r, store_sem):
    g, me = lax.axis_index("dp"), lax.axis_index("sp")
    chip, core = me // 2, me % 2
    far = (1 - chip) * 2
    partner, cross = chip * 2 + 1 - core, far + core
    turned_core = core + g - 2 * core * g
    wx = far + turned_core
    wx_other = far + 1 - turned_core
    peer = (1 - g, me)
    weights = (wq_ref, wk_ref, wv_ref)

    def remote(src, dst, send, recv, to):
        return pltpu.make_async_remote_copy(src, dst, send, recv, device_id=to, device_id_type=MESH)

    barrier = pltpu.get_barrier_semaphore()
    for to in ((g, partner), (g, cross), (g, far + 1 - core), peer):
        pl.semaphore_signal(barrier, inc=1, device_id=to, device_id_type=MESH)
    pl.semaphore_wait(barrier, 4)

    def away(owner):
        return (owner - me + 3) % 4 % 3

    def w_cross(n, to, rows_of):
        m, half = n // 2, n % 2
        return remote(weights[m].at[pl.ds(half * 256, 256), _rows(to, WIDE)],
                      w_s.at[m, pl.ds(pl.multiple_of(rows_of * 512 + half * 256, 256), 256)], wx_s.at[n], wx_r.at[n], (g, to))

    def w_trade(n, rows_of):
        m, half = n // 2, n % 2
        at = w_s.at[m, pl.ds(pl.multiple_of(rows_of * 512 + half * 256, 256), 256)]
        return remote(at, at, wy_s.at[n], wy_r.at[n], peer)

    def w_partner(m, rows_of):
        return remote(weights[m].at[:, _rows(partner, WIDE)], w_s.at[m, _rows(rows_of, 512)], wp_s.at[m], wp_r.at[m], (g, partner))

    def a_piece(n, send, recv, to):
        at = a_s.at[_rows(n, PIECE)]
        return remote(at, at, send, recv, to)

    def wo_part(rows_of, part):
        return wo_s.at[pl.ds(pl.multiple_of(rows_of * 512 + part * 256, 256), 256)]

    def wo_cross(rows_of):
        return remote(wo_ref.at[_rows(g, 256)], wo_part(rows_of, g), ox_s, ox_r, (g, cross))

    def wo_trade(part):
        at = wo_part(cross, part)
        return remote(at, at, oy_s, oy_r, peer)

    def wo_forward(rows_of, part, n):
        at = wo_part(rows_of, part)
        return remote(at, at, of_s.at[n], of_r.at[n], (g, partner))

    def wo_partner(rows_of):
        return remote(wo_ref, wo_s.at[_rows(rows_of, 512)], op_s, op_r, (g, partner))

    def result(n, source, to):
        return remote(out_s.at[_rows(away(n // 4) * 4 + n % 4, PIECE)], seen_s.at[_rows(n % 4, PIECE), _rows(source, WIDE)], s_s.at[n], s_r.at[source, n % 4], (g, to))

    load_x = [pltpu.make_async_copy(x_ref.at[pl.ds(n * PIECE, PIECE)], a_s.at[_rows(me * 4 + n, PIECE)], load_sem.at[n]) for n in range(4)]
    load_small = [pltpu.make_async_copy(a, b, load_sem.at[12 + n]) for n, (a, b) in enumerate(((gain_hbm, gain_ref), (near_hbm, near_ref), (far_hbm, far_ref)))]
    load_w = [pltpu.make_async_copy(weights[m].at[:, _rows(me, WIDE)], w_s.at[m, _rows(me, 512)], load_sem.at[4 + m]) for m in range(3)]
    load_wo = pltpu.make_async_copy(wo_ref, wo_s.at[_rows(me, 512)], load_sem.at[7])
    again_x = [pltpu.make_async_copy(x_ref.at[pl.ds(n * PIECE, PIECE)], a_s.at[_rows(me * 4 + n, PIECE)], load_sem.at[8 + n]) for n in range(4)]

    def store(n, j):
        at = _rows(j, TILE)
        return pltpu.make_async_copy(a_s.at[_rows(me * 4 + n, PIECE), at], y_ref.at[_rows(n, PIECE), at], store_sem.at[n, j])

    for n in range(6):
        w_cross(n, wx, me).start()
    for copy in load_small + load_x:
        copy.start()
    for m in range(3):
        w_partner(m, me).start()
    for copy in load_w:
        copy.start()

    for copy in load_small:
        copy.wait()
    for n in range(4):
        load_x[n].wait()
        mine = _rows(me * 4 + n, PIECE)
        wide = a_s[mine, :].astype(jnp.float32)
        scale = lax.rsqrt(jnp.mean(wide * wide, -1, keepdims=True) + 1e-6)
        a_s[mine, :] = (wide * scale * gain_ref[...].astype(jnp.float32)[None, :]).astype(jnp.bfloat16)
        a_piece(me * 4 + n, ap_s.at[n], ap_r.at[n], (g, partner)).start()
    for n in range(4):
        a_piece(partner * 4 + n, ap_s.at[n], ap_r.at[n], (g, partner)).wait_recv()
    for r in range(4):
        a_piece(chip * 8 + 2 * r + core, ax_s.at[r], ax_r.at[r], (g, cross)).start()
    wo_cross(me).start()
    wo_partner(me).start()
    load_wo.start()

    for n in range(6):
        w_cross(n, me, wx).wait_recv()
        w_trade(n, wx).start()
    for copy in load_w:
        copy.wait()
    for m in range(3):
        w_partner(m, partner).wait_recv()
    for n in range(6):
        w_trade(n, wx_other).wait_recv()

    v_s[:, HEAD:, :] = jnp.ones((HEADS, SUMS, ROWS), jnp.bfloat16)

    def q_rows(n):
        return _rows(jnp.where(n // 4 == chip, n % 4, 4), CHUNK)

    def project(n):
        rows = _rows(n, CHUNK)
        cos, sin = [], []
        for s in range(2):
            near_cos, near_sin = near_ref[0], near_ref[1]
            far_cos, far_sin = far_ref[0, pl.ds(2 * n + s, 1), :], far_ref[1, pl.ds(2 * n + s, 1), :]
            cos.append(far_cos * near_cos - far_sin * near_sin)
            sin.append(far_sin * near_cos + far_cos * near_sin)
        cos, sin = jnp.concatenate(cos, 0), jnp.concatenate(sin, 0)
        for m, to in ((0, q_s), (1, k_s)):
            got = _dot(a_s[rows, :], w_s[m], 1, 0).astype(jnp.bfloat16).astype(jnp.float32)
            for h in range(HEADS):
                t = got[:, h * HEAD : (h + 1) * HEAD]
                to[h, q_rows(n) if m == 0 else rows, :] = (t * cos + pltpu.roll(t, HEAD // 2, 1) * sin).astype(jnp.bfloat16)
        got = _dot(a_s[rows, :], w_s[2], 1, 0)
        for h in range(HEADS):
            v_s[h, :HEAD, rows] = got[:, h * HEAD : (h + 1) * HEAD].T.astype(jnp.bfloat16)

    e = HEAD**-0.5 * LOG2E

    def attend(n):
        top_s[...] = jnp.full(top_s.shape, NEG, jnp.float32)
        mix_s[...] = jnp.zeros(mix_s.shape, jnp.float32)
        def block(j, masked):
            keys = _rows(j, CHUNK)
            scores = [_dot(k_s[h, keys, :], q_s[h, q_rows(n), :], 1, 1) for h in range(HEADS)]
            if masked:
                ok = lax.broadcasted_iota(jnp.int32, (CHUNK, CHUNK), 1) >= lax.broadcasted_iota(jnp.int32, (CHUNK, CHUNK), 0)
            weights, keeps = [], []
            for h, s in enumerate(scores):
                if masked:
                    s = jnp.where(ok, s, HIDDEN)
                old = top_s[h : h + 1, :]
                top = jnp.maximum(old, s.max(axis=0, keepdims=True))
                top_s[h : h + 1, :] = top
                weights.append(jnp.exp2((s - top) * e).astype(jnp.bfloat16))
                keeps.append(jnp.exp2((old - top) * e))
            for h in range(HEADS):
                mix_s[h] = mix_s[h] * keeps[h] + _dot(v_s[h, :, keys], weights[h], 1, 0)

        lax.fori_loop(0, n, lambda j, _: block(j, False), None)
        block(n, True)

    def results():
        each = []
        for h in range(HEADS):
            total = mix_s[h, HEAD : HEAD + 1, :]
            each.append((mix_s[h, :HEAD, :] * (1 / total)).T.astype(jnp.bfloat16))
        return jnp.concatenate(each, axis=1)

    def pass_wo_on():
        wo_cross(cross).wait_recv()
        wo_trade(g).start()
        wo_forward(cross, g, 0).start()

    lax.fori_loop(0, 4, lambda r, _: project(chip * 4 + r), None)

    def step(n, _):
        r, owner = n % 4, n // 2

        @pl.when(n // 4 != chip)
        def _():
            mine = far * 4 + 2 * r + core
            a_piece(mine, ax_s.at[r], ax_r.at[r], (g, cross)).wait_recv()
            a_piece(mine, af_s.at[r], af_r.at[r], (g, partner)).start()
            a_piece(far * 4 + 2 * r + 1 - core, af_s.at[r], af_r.at[r], (g, partner)).wait_recv()
            project(n)

        @pl.when((n == 6) & (chip == 1))
        def _():
            pass_wo_on()

        attend(n)

        @pl.when(owner == me)
        def _():
            seen_s[_rows(n % 2, CHUNK), _rows(me, WIDE)] = results()

        @pl.when(owner != me)
        def _():
            out_s[_rows(away(owner) * 2 + n % 2, CHUNK), :] = results()
            result(2 * n, me, owner).start()
            result(2 * n + 1, me, owner).start()

    lax.fori_loop(0, 8, step, None)

    for r in range(4):
        a_piece(me * 4 + r, ap_s.at[r], ap_r.at[r], (g, partner)).wait_send()
        a_piece(chip * 8 + 2 * r + core, ax_s.at[r], ax_r.at[r], (g, cross)).wait_send()
    for copy in again_x:
        copy.start()

    @pl.when(chip == 0)
    def _():
        pass_wo_on()

    wo_trade(1 - g).wait_recv()
    wo_forward(cross, 1 - g, 1).start()
    load_wo.wait()
    wo_partner(partner).wait_recv()
    for n in range(2):
        part = g if n == 0 else 1 - g
        wo_forward(far + 1 - core, part, n).wait_recv()
    for copy in again_x:
        copy.wait()

    def arrive(n, *others):
        for other in others:
            result(me * 4 + n, other, me).wait_recv()

    def product(n, j, start, depth):
        part = pl.ds(pl.multiple_of(start, OWN), depth)
        return _dot(seen_s[_rows(n, PIECE), part], wo_s[part, _rows(j, TILE)], 1, 0)

    def put(n, j, y):
        mine, at = _rows(me * 4 + n, PIECE), _rows(j, TILE)
        a_s[mine, at] = (a_s[mine, at].astype(jnp.float32) + y).astype(jnp.bfloat16)
        store(n, j).start()

    def whole(n, _):
        arrive(n, partner, cross, far + 1 - core)
        lax.fori_loop(0, D // TILE, lambda j, _: put(n, j, product(n, j, 0, D)), None)

    lax.fori_loop(0, 3, whole, None)

    arrive(3, partner)

    def near(j, _):
        part_s[:, _rows(j, TILE)] = product(3, j, chip * OWN, OWN)

    lax.fori_loop(0, D // TILE, near, None)
    arrive(3, cross, far + 1 - core)
    lax.fori_loop(0, D // TILE, lambda j, _: put(3, j, part_s[:, _rows(j, TILE)] + product(3, j, far * WIDE, OWN)), None)

    for n in range(6):
        w_cross(n, wx, me).wait_send()
        w_trade(n, wx).wait_send()
    for m in range(3):
        w_partner(m, me).wait_send()
    for r in range(4):
        a_piece(far * 4 + 2 * r + core, af_s.at[r], af_r.at[r], (g, partner)).wait_send()
    wo_cross(me).wait_send()
    wo_partner(me).wait_send()
    wo_trade(g).wait_send()
    wo_forward(cross, g, 0).wait_send()
    wo_forward(cross, 1 - g, 1).wait_send()

    def sent(n, _):
        @pl.when(n // 4 != me)
        def _():
            result(n, me, n // 4).wait_send()

    lax.fori_loop(0, 16, sent, None)
    for n in range(4):
        for j in range(D // TILE):
            store(n, j).wait()


def _take(here_ref, y_ref, held, load, store):
    part = OWN // held.shape[0]
    loads = [pltpu.make_async_copy(here_ref.at[pl.ds(n * part, part)], held.at[n], load.at[n]) for n in range(held.shape[0])]
    stores = [pltpu.make_async_copy(held.at[n], y_ref.at[pl.ds(n * part, part)], store.at[n]) for n in range(held.shape[0])]
    for copy in loads:
        copy.start()
    for got, put in zip(loads, stores):
        got.wait()
        put.start()
    for copy in stores:
        copy.wait()


def _turns(places):
    half = HEAD // 2
    angle = places[:, None].astype(np.float64) * THETA ** (-np.arange(half) / half)
    cos, sin = np.cos(angle), np.sin(angle)
    return np.stack([np.concatenate([cos, cos], 1), np.concatenate([-sin, sin], 1)]).astype(np.float32)


def solution(mesh):
    def step(x, gain, wq, wk, wv, wo):
        any_ = pl.BlockSpec(memory_space=pl.ANY)
        bf16, dma = jnp.bfloat16, pltpu.SemaphoreType.DMA
        here = pl.pallas_call(
            _kernel,
            out_shape=jax.ShapeDtypeStruct((OWN, D), bf16),
            in_specs=[any_] * 8,
            out_specs=any_,
            scratch_shapes=[
                pltpu.VMEM((D,), bf16),
                pltpu.VMEM((2, PIECE, HEAD), jnp.float32),
                pltpu.VMEM((2, ROWS // PIECE, HEAD), jnp.float32),
                pltpu.VMEM((ROWS, D), bf16),
                pltpu.VMEM((3, D, WIDE), bf16),
                pltpu.VMEM((D, D), bf16),
                pltpu.VMEM((HEADS, 5 * CHUNK, HEAD), bf16),
                pltpu.VMEM((HEADS, ROWS, HEAD), bf16),
                pltpu.VMEM((HEADS, HEAD + SUMS, ROWS), bf16),
                pltpu.VMEM((ROWS - OWN, WIDE), bf16),
                pltpu.VMEM((OWN, D), bf16),
                pltpu.VMEM((PIECE, D), jnp.float32),
                pltpu.VMEM((HEADS, CHUNK), jnp.float32),
                pltpu.VMEM((HEADS, HEAD + SUMS, CHUNK), jnp.float32),
                dma((15,)),
                dma((6,)), dma((6,)), dma((6,)), dma((6,)), dma((3,)), dma((3,)),
                dma((4,)), dma((4,)), dma((4,)), dma((4,)), dma((4,)), dma((4,)),
                dma, dma, dma, dma, dma, dma, dma((2,)), dma((2,)),
                dma((16,)), dma((4, 4)), dma((4, D // TILE)),
            ],
            compiler_params=pltpu.CompilerParams(collective_id=0, has_side_effects=True, vmem_limit_bytes=67043328),
        )(x, gain, wq, wk, wv, wo, jnp.asarray(_turns(np.arange(PIECE))), jnp.asarray(_turns(np.arange(ROWS // PIECE) * PIECE)))
        parts = 8
        return pl.pallas_call(
            _take,
            out_shape=jax.ShapeDtypeStruct((OWN, D), bf16),
            in_specs=[any_],
            out_specs=any_,
            scratch_shapes=[pltpu.VMEM((parts, OWN // parts, D), bf16), dma((parts,)), dma((parts,))],
        )(here)

    tokens, whole = P(("dp", "sp"), None), P("sp", None)
    return jax.shard_map(
        step,
        mesh=mesh,
        in_specs=(tokens, P(None), whole, whole, whole, whole),
        out_specs=tokens,
        check_vma=False,
    )
```

```python
import functools

import numpy as np

import jax
import jax.numpy as jnp
from jax import lax
from jax.experimental import pallas as pl
from jax.experimental.pallas import tpu as pltpu
from jax.sharding import PartitionSpec as P

MESH = pl.DeviceIdType.MESH
HEAD = 128
THETA = 10000
NEG = -1e30
HIDDEN = 2 * NEG
LOG2E = 1.4426950408889634
DEVICES = 4
OWN = 1024
ROWS = DEVICES * OWN
D = 2048
HEADS = 4
WIDE = HEADS * HEAD
PIECE = 256
TILE = 1024
CHUNK = 512
SUMS = 16


def _dot(a, b, ca, cb):
    return lax.dot_general(a, b, (((ca,), (cb,)), ((), ())), preferred_element_type=jnp.float32)


def _rows(i, size):
    return pl.ds(pl.multiple_of(i * size, size), size)


def _kernel(x_ref, gain_hbm, wq_ref, wk_ref, wv_ref, wo_ref, near_hbm, far_hbm, y_ref, gain_ref, near_ref, far_ref,
            a_s, w_s, wo_s, q_s, k_s, v_s, out_s, seen_s, part_s, top_s, mix_s,
            load_sem, wx_s, wx_r, wy_s, wy_r, wp_s, wp_r, ap_s, ap_r, ax_s, ax_r, af_s, af_r,
            op_s, op_r, ox_s, ox_r, oy_s, oy_r, of_s, of_r, s_s, s_r, store_sem):
    g, me = lax.axis_index("dp"), lax.axis_index("sp")
    chip, core = me // 2, me % 2
    far = (1 - chip) * 2
    partner, cross = chip * 2 + 1 - core, far + core
    turned_core = core + g - 2 * core * g
    wx = far + turned_core
    wx_other = far + 1 - turned_core
    peer = (1 - g, me)
    weights = (wq_ref, wk_ref, wv_ref)

    def remote(src, dst, send, recv, to):
        return pltpu.make_async_remote_copy(src, dst, send, recv, device_id=to, device_id_type=MESH)

    barrier = pltpu.get_barrier_semaphore()
    for to in ((g, partner), (g, cross), (g, far + 1 - core), peer):
        pl.semaphore_signal(barrier, inc=1, device_id=to, device_id_type=MESH)
    pl.semaphore_wait(barrier, 4)

    def away(owner):
        return (owner - me + 3) % 4 % 3

    def w_cross(n, to, rows_of):
        m, half = n // 2, n % 2
        return remote(weights[m].at[pl.ds(half * 256, 256), _rows(to, WIDE)],
                      w_s.at[m, pl.ds(pl.multiple_of(rows_of * 512 + half * 256, 256), 256)], wx_s.at[n], wx_r.at[n], (g, to))

    def w_trade(n, rows_of):
        m, half = n // 2, n % 2
        at = w_s.at[m, pl.ds(pl.multiple_of(rows_of * 512 + half * 256, 256), 256)]
        return remote(at, at, wy_s.at[n], wy_r.at[n], peer)

    def w_partner(m, rows_of):
        return remote(weights[m].at[:, _rows(partner, WIDE)], w_s.at[m, _rows(rows_of, 512)], wp_s.at[m], wp_r.at[m], (g, partner))

    def a_piece(n, send, recv, to):
        at = a_s.at[_rows(n, PIECE)]
        return remote(at, at, send, recv, to)

    def wo_part(rows_of, part):
        return wo_s.at[pl.ds(pl.multiple_of(rows_of * 512 + part * 256, 256), 256)]

    def wo_cross(rows_of):
        return remote(wo_ref.at[_rows(g, 256)], wo_part(rows_of, g), ox_s, ox_r, (g, cross))

    def wo_trade(part):
        at = wo_part(cross, part)
        return remote(at, at, oy_s, oy_r, peer)

    def wo_forward(rows_of, part, n):
        at = wo_part(rows_of, part)
        return remote(at, at, of_s.at[n], of_r.at[n], (g, partner))

    def wo_partner(rows_of):
        return remote(wo_ref, wo_s.at[_rows(rows_of, 512)], op_s, op_r, (g, partner))

    def result(n, source, to):
        return remote(out_s.at[_rows(away(n // 4) * 4 + n % 4, PIECE)], seen_s.at[_rows(n % 4, PIECE), _rows(source, WIDE)], s_s.at[n], s_r.at[source, n % 4], (g, to))

    load_x = [pltpu.make_async_copy(x_ref.at[pl.ds(n * PIECE, PIECE)], a_s.at[_rows(me * 4 + n, PIECE)], load_sem.at[n]) for n in range(4)]
    load_small = [pltpu.make_async_copy(a, b, load_sem.at[12 + n]) for n, (a, b) in enumerate(((gain_hbm, gain_ref), (near_hbm, near_ref), (far_hbm, far_ref)))]
    load_w = [pltpu.make_async_copy(weights[m].at[:, _rows(me, WIDE)], w_s.at[m, _rows(me, 512)], load_sem.at[4 + m]) for m in range(3)]
    load_wo = pltpu.make_async_copy(wo_ref, wo_s.at[_rows(me, 512)], load_sem.at[7])
    again_x = [pltpu.make_async_copy(x_ref.at[pl.ds(n * PIECE, PIECE)], a_s.at[_rows(me * 4 + n, PIECE)], load_sem.at[8 + n]) for n in range(4)]

    def store(n, j):
        at = _rows(j, TILE)
        return pltpu.make_async_copy(a_s.at[_rows(me * 4 + n, PIECE), at], y_ref.at[_rows(n, PIECE), at], store_sem.at[n, j])

    for n in range(6):
        w_cross(n, wx, me).start()
    for copy in load_small + load_x:
        copy.start()
    for m in range(3):
        w_partner(m, me).start()
    for copy in load_w:
        copy.start()

    for copy in load_small:
        copy.wait()
    for n in range(4):
        load_x[n].wait()
        mine = _rows(me * 4 + n, PIECE)
        wide = a_s[mine, :].astype(jnp.float32)
        scale = lax.rsqrt(jnp.mean(wide * wide, -1, keepdims=True) + 1e-6)
        a_s[mine, :] = (wide * scale * gain_ref[...].astype(jnp.float32)[None, :]).astype(jnp.bfloat16)
        a_piece(me * 4 + n, ap_s.at[n], ap_r.at[n], (g, partner)).start()
    for n in range(4):
        a_piece(partner * 4 + n, ap_s.at[n], ap_r.at[n], (g, partner)).wait_recv()
    for r in range(4):
        a_piece(chip * 8 + 2 * r + core, ax_s.at[r], ax_r.at[r], (g, cross)).start()
    wo_cross(me).start()
    wo_partner(me).start()
    load_wo.start()

    for n in range(6):
        w_cross(n, me, wx).wait_recv()
        w_trade(n, wx).start()
    for copy in load_w:
        copy.wait()
    for m in range(3):
        w_partner(m, partner).wait_recv()
    for n in range(6):
        w_trade(n, wx_other).wait_recv()

    v_s[:, HEAD:, :] = jnp.ones((HEADS, SUMS, ROWS), jnp.bfloat16)

    def q_rows(n):
        return _rows(jnp.where(n // 4 == chip, n % 4, 4), CHUNK)

    def project(n):
        rows = _rows(n, CHUNK)
        cos, sin = [], []
        for s in range(2):
            near_cos, near_sin = near_ref[0], near_ref[1]
            far_cos, far_sin = far_ref[0, pl.ds(2 * n + s, 1), :], far_ref[1, pl.ds(2 * n + s, 1), :]
            cos.append(far_cos * near_cos - far_sin * near_sin)
            sin.append(far_sin * near_cos + far_cos * near_sin)
        cos, sin = jnp.concatenate(cos, 0), jnp.concatenate(sin, 0)
        for m, to in ((0, q_s), (1, k_s)):
            got = _dot(a_s[rows, :], w_s[m], 1, 0).astype(jnp.bfloat16).astype(jnp.float32)
            for h in range(HEADS):
                t = got[:, h * HEAD : (h + 1) * HEAD]
                to[h, q_rows(n) if m == 0 else rows, :] = (t * cos + pltpu.roll(t, HEAD // 2, 1) * sin).astype(jnp.bfloat16)
        got = _dot(a_s[rows, :], w_s[2], 1, 0)
        for h in range(HEADS):
            v_s[h, :HEAD, rows] = got[:, h * HEAD : (h + 1) * HEAD].T.astype(jnp.bfloat16)

    e = HEAD**-0.5 * LOG2E

    def attend(n):
        top_s[...] = jnp.full(top_s.shape, NEG, jnp.float32)
        mix_s[...] = jnp.zeros(mix_s.shape, jnp.float32)
        def block(j, masked):
            keys = _rows(j, CHUNK)
            scores = [_dot(k_s[h, keys, :], q_s[h, q_rows(n), :], 1, 1) for h in range(HEADS)]
            if masked:
                ok = lax.broadcasted_iota(jnp.int32, (CHUNK, CHUNK), 1) >= lax.broadcasted_iota(jnp.int32, (CHUNK, CHUNK), 0)
            weights, keeps = [], []
            for h, s in enumerate(scores):
                if masked:
                    s = jnp.where(ok, s, HIDDEN)
                old = top_s[h : h + 1, :]
                top = jnp.maximum(old, s.max(axis=0, keepdims=True))
                top_s[h : h + 1, :] = top
                weights.append(jnp.exp2((s - top) * e).astype(jnp.bfloat16))
                keeps.append(jnp.exp2((old - top) * e))
            for h in range(HEADS):
                mix_s[h] = mix_s[h] * keeps[h] + _dot(v_s[h, :, keys], weights[h], 1, 0)

        lax.fori_loop(0, n, lambda j, _: block(j, False), None)
        block(n, True)

    def results():
        each = []
        for h in range(HEADS):
            total = mix_s[h, HEAD : HEAD + 1, :]
            each.append((mix_s[h, :HEAD, :] * (1 / total)).T.astype(jnp.bfloat16))
        return jnp.concatenate(each, axis=1)

    def pass_wo_on():
        wo_cross(cross).wait_recv()
        wo_trade(g).start()
        wo_forward(cross, g, 0).start()

    lax.fori_loop(0, 4, lambda r, _: project(chip * 4 + r), None)

    def step(n, _):
        r, owner = n % 4, n // 2

        @pl.when(n // 4 != chip)
        def _():
            mine = far * 4 + 2 * r + core
            a_piece(mine, ax_s.at[r], ax_r.at[r], (g, cross)).wait_recv()
            a_piece(mine, af_s.at[r], af_r.at[r], (g, partner)).start()
            a_piece(far * 4 + 2 * r + 1 - core, af_s.at[r], af_r.at[r], (g, partner)).wait_recv()
            project(n)

        @pl.when((n == 6) & (chip == 1))
        def _():
            pass_wo_on()

        attend(n)

        @pl.when(owner == me)
        def _():
            seen_s[_rows(n % 2, CHUNK), _rows(me, WIDE)] = results()

        @pl.when(owner != me)
        def _():
            out_s[_rows(away(owner) * 2 + n % 2, CHUNK), :] = results()
            result(2 * n, me, owner).start()
            result(2 * n + 1, me, owner).start()

    lax.fori_loop(0, 8, step, None)

    for r in range(4):
        a_piece(me * 4 + r, ap_s.at[r], ap_r.at[r], (g, partner)).wait_send()
        a_piece(chip * 8 + 2 * r + core, ax_s.at[r], ax_r.at[r], (g, cross)).wait_send()
    for copy in again_x:
        copy.start()

    @pl.when(chip == 0)
    def _():
        pass_wo_on()

    wo_trade(1 - g).wait_recv()
    wo_forward(cross, 1 - g, 1).start()
    load_wo.wait()
    wo_partner(partner).wait_recv()
    for n in range(2):
        part = g if n == 0 else 1 - g
        wo_forward(far + 1 - core, part, n).wait_recv()
    for copy in again_x:
        copy.wait()

    def arrive(n, *others):
        for other in others:
            result(me * 4 + n, other, me).wait_recv()

    def product(n, j, start, depth):
        part = pl.ds(pl.multiple_of(start, OWN), depth)
        return _dot(seen_s[_rows(n, PIECE), part], wo_s[part, _rows(j, TILE)], 1, 0)

    def put(n, j, y):
        mine, at = _rows(me * 4 + n, PIECE), _rows(j, TILE)
        a_s[mine, at] = (a_s[mine, at].astype(jnp.float32) + y).astype(jnp.bfloat16)
        store(n, j).start()

    def whole(n, _):
        arrive(n, partner, cross, far + 1 - core)
        lax.fori_loop(0, D // TILE, lambda j, _: put(n, j, product(n, j, 0, D)), None)

    lax.fori_loop(0, 3, whole, None)

    arrive(3, partner)

    def near(j, _):
        part_s[:, _rows(j, TILE)] = product(3, j, chip * OWN, OWN)

    lax.fori_loop(0, D // TILE, near, None)
    arrive(3, cross, far + 1 - core)
    lax.fori_loop(0, D // TILE, lambda j, _: put(3, j, part_s[:, _rows(j, TILE)] + product(3, j, far * WIDE, OWN)), None)

    for n in range(6):
        w_cross(n, wx, me).wait_send()
        w_trade(n, wx).wait_send()
    for m in range(3):
        w_partner(m, me).wait_send()
    for r in range(4):
        a_piece(far * 4 + 2 * r + core, af_s.at[r], af_r.at[r], (g, partner)).wait_send()
    wo_cross(me).wait_send()
    wo_partner(me).wait_send()
    wo_trade(g).wait_send()
    wo_forward(cross, g, 0).wait_send()
    wo_forward(cross, 1 - g, 1).wait_send()

    def sent(n, _):
        @pl.when(n // 4 != me)
        def _():
            result(n, me, n // 4).wait_send()

    lax.fori_loop(0, 16, sent, None)
    for n in range(4):
        for j in range(D // TILE):
            store(n, j).wait()


def _take(here_ref, y_ref, held, load, store):
    part = OWN // held.shape[0]
    loads = [pltpu.make_async_copy(here_ref.at[pl.ds(n * part, part)], held.at[n], load.at[n]) for n in range(held.shape[0])]
    stores = [pltpu.make_async_copy(held.at[n], y_ref.at[pl.ds(n * part, part)], store.at[n]) for n in range(held.shape[0])]
    for copy in loads:
        copy.start()
    for got, put in zip(loads, stores):
        got.wait()
        put.start()
    for copy in stores:
        copy.wait()


def _turns(places):
    half = HEAD // 2
    angle = places[:, None].astype(np.float64) * THETA ** (-np.arange(half) / half)
    cos, sin = np.cos(angle), np.sin(angle)
    return np.stack([np.concatenate([cos, cos], 1), np.concatenate([-sin, sin], 1)]).astype(np.float32)


def solution(mesh):
    def step(x, gain, wq, wk, wv, wo):
        any_ = pl.BlockSpec(memory_space=pl.ANY)
        bf16, dma = jnp.bfloat16, pltpu.SemaphoreType.DMA
        here = pl.pallas_call(
            _kernel,
            out_shape=jax.ShapeDtypeStruct((OWN, D), bf16),
            in_specs=[any_] * 8,
            out_specs=any_,
            scratch_shapes=[
                pltpu.VMEM((D,), bf16),
                pltpu.VMEM((2, PIECE, HEAD), jnp.float32),
                pltpu.VMEM((2, ROWS // PIECE, HEAD), jnp.float32),
                pltpu.VMEM((ROWS, D), bf16),
                pltpu.VMEM((3, D, WIDE), bf16),
                pltpu.VMEM((D, D), bf16),
                pltpu.VMEM((HEADS, 5 * CHUNK, HEAD), bf16),
                pltpu.VMEM((HEADS, ROWS, HEAD), bf16),
                pltpu.VMEM((HEADS, HEAD + SUMS, ROWS), bf16),
                pltpu.VMEM((ROWS - OWN, WIDE), bf16),
                pltpu.VMEM((OWN, D), bf16),
                pltpu.VMEM((PIECE, D), jnp.float32),
                pltpu.VMEM((HEADS, CHUNK), jnp.float32),
                pltpu.VMEM((HEADS, HEAD + SUMS, CHUNK), jnp.float32),
                dma((15,)),
                dma((6,)), dma((6,)), dma((6,)), dma((6,)), dma((3,)), dma((3,)),
                dma((4,)), dma((4,)), dma((4,)), dma((4,)), dma((4,)), dma((4,)),
                dma, dma, dma, dma, dma, dma, dma((2,)), dma((2,)),
                dma((16,)), dma((4, 4)), dma((4, D // TILE)),
            ],
            compiler_params=pltpu.CompilerParams(collective_id=0, has_side_effects=True, vmem_limit_bytes=67043328),
        )(x, gain, wq, wk, wv, wo, jnp.asarray(_turns(np.arange(PIECE))), jnp.asarray(_turns(np.arange(ROWS // PIECE) * PIECE)))
        parts = 4
        return pl.pallas_call(
            _take,
            out_shape=jax.ShapeDtypeStruct((OWN, D), bf16),
            in_specs=[any_],
            out_specs=any_,
            scratch_shapes=[pltpu.VMEM((parts, OWN // parts, D), bf16), dma((parts,)), dma((parts,))],
        )(here)

    tokens, whole = P(("dp", "sp"), None), P("sp", None)
    return jax.shard_map(
        step,
        mesh=mesh,
        in_specs=(tokens, P(None), whole, whole, whole, whole),
        out_specs=tokens,
        check_vma=False,
    )
```

```python
import functools

import numpy as np

import jax
import jax.numpy as jnp
from jax import lax
from jax.experimental import pallas as pl
from jax.experimental.pallas import tpu as pltpu
from jax.sharding import PartitionSpec as P

MESH = pl.DeviceIdType.MESH
HEAD = 128
THETA = 10000
NEG = -1e30
HIDDEN = 2 * NEG
LOG2E = 1.4426950408889634
DEVICES = 4
OWN = 1024
ROWS = DEVICES * OWN
D = 2048
HEADS = 4
WIDE = HEADS * HEAD
PIECE = 256
TILE = 2048
CHUNK = 512
SUMS = 16


def _dot(a, b, ca, cb):
    return lax.dot_general(a, b, (((ca,), (cb,)), ((), ())), preferred_element_type=jnp.float32)


def _rows(i, size):
    return pl.ds(pl.multiple_of(i * size, size), size)


def _kernel(x_ref, gain_hbm, wq_ref, wk_ref, wv_ref, wo_ref, near_hbm, far_hbm, y_ref, gain_ref, near_ref, far_ref,
            a_s, w_s, wo_s, q_s, k_s, v_s, out_s, seen_s, part_s, top_s, mix_s,
            load_sem, wx_s, wx_r, wy_s, wy_r, wp_s, wp_r, ap_s, ap_r, ax_s, ax_r, af_s, af_r,
            op_s, op_r, ox_s, ox_r, oy_s, oy_r, of_s, of_r, s_s, s_r, store_sem):
    g, me = lax.axis_index("dp"), lax.axis_index("sp")
    chip, core = me // 2, me % 2
    far = (1 - chip) * 2
    partner, cross = chip * 2 + 1 - core, far + core
    turned_core = core + g - 2 * core * g
    wx = far + turned_core
    wx_other = far + 1 - turned_core
    peer = (1 - g, me)
    weights = (wq_ref, wk_ref, wv_ref)

    def remote(src, dst, send, recv, to):
        return pltpu.make_async_remote_copy(src, dst, send, recv, device_id=to, device_id_type=MESH)

    barrier = pltpu.get_barrier_semaphore()
    for to in ((g, cross), (g, far + 1 - core), peer, (g, partner)):
        pl.semaphore_signal(barrier, inc=1, device_id=to, device_id_type=MESH)
    pl.semaphore_wait(barrier, 4)

    def away(owner):
        return (owner - me + 3) % 4 % 3

    def w_cross(n, to, rows_of):
        m, half = n // 2, n % 2
        return remote(weights[m].at[pl.ds(half * 256, 256), _rows(to, WIDE)],
                      w_s.at[m, pl.ds(pl.multiple_of(rows_of * 512 + half * 256, 256), 256)], wx_s.at[n], wx_r.at[n], (g, to))

    def w_trade(n, rows_of):
        m, half = n // 2, n % 2
        at = w_s.at[m, pl.ds(pl.multiple_of(rows_of * 512 + half * 256, 256), 256)]
        return remote(at, at, wy_s.at[n], wy_r.at[n], peer)

    def w_partner(m, rows_of):
        return remote(weights[m].at[:, _rows(partner, WIDE)], w_s.at[m, _rows(rows_of, 512)], wp_s.at[m], wp_r.at[m], (g, partner))

    def a_piece(n, send, recv, to):
        at = a_s.at[_rows(n, PIECE)]
        return remote(at, at, send, recv, to)

    def wo_part(rows_of, part):
        return wo_s.at[pl.ds(pl.multiple_of(rows_of * 512 + part * 256, 256), 256)]

    def wo_cross(rows_of):
        return remote(wo_ref.at[_rows(g, 256)], wo_part(rows_of, g), ox_s, ox_r, (g, cross))

    def wo_trade(part):
        at = wo_part(cross, part)
        return remote(at, at, oy_s, oy_r, peer)

    def wo_forward(rows_of, part, n):
        at = wo_part(rows_of, part)
        return remote(at, at, of_s.at[n], of_r.at[n], (g, partner))

    def wo_partner(rows_of):
        return remote(wo_ref, wo_s.at[_rows(rows_of, 512)], op_s, op_r, (g, partner))

    def result(n, source, to):
        return remote(out_s.at[_rows(away(n // 4) * 4 + n % 4, PIECE)], seen_s.at[_rows(n % 4, PIECE), _rows(source, WIDE)], s_s.at[n], s_r.at[source, n % 4], (g, to))

    load_x = [pltpu.make_async_copy(x_ref.at[pl.ds(n * PIECE, PIECE)], a_s.at[_rows(me * 4 + n, PIECE)], load_sem.at[n]) for n in range(4)]
    load_small = [pltpu.make_async_copy(a, b, load_sem.at[12 + n]) for n, (a, b) in enumerate(((gain_hbm, gain_ref), (near_hbm, near_ref), (far_hbm, far_ref)))]
    load_w = [pltpu.make_async_copy(weights[m].at[:, _rows(me, WIDE)], w_s.at[m, _rows(me, 512)], load_sem.at[4 + m]) for m in range(3)]
    load_wo = pltpu.make_async_copy(wo_ref, wo_s.at[_rows(me, 512)], load_sem.at[7])
    again_x = [pltpu.make_async_copy(x_ref.at[pl.ds(n * PIECE, PIECE)], a_s.at[_rows(me * 4 + n, PIECE)], load_sem.at[8 + n]) for n in range(4)]

    def store(n, j):
        at = _rows(j, TILE)
        return pltpu.make_async_copy(a_s.at[_rows(me * 4 + n, PIECE), at], y_ref.at[_rows(n, PIECE), at], store_sem.at[n, j])

    for n in range(6):
        w_cross(n, wx, me).start()
    for copy in load_small + load_x:
        copy.start()
    for m in range(3):
        w_partner(m, me).start()
    for copy in load_w:
        copy.start()

    for copy in load_small:
        copy.wait()
    for n in range(4):
        load_x[n].wait()
        mine = _rows(me * 4 + n, PIECE)
        wide = a_s[mine, :].astype(jnp.float32)
        scale = lax.rsqrt(jnp.mean(wide * wide, -1, keepdims=True) + 1e-6)
        a_s[mine, :] = (wide * scale * gain_ref[...].astype(jnp.float32)[None, :]).astype(jnp.bfloat16)
        a_piece(me * 4 + n, ap_s.at[n], ap_r.at[n], (g, partner)).start()
    for n in range(4):
        a_piece(partner * 4 + n, ap_s.at[n], ap_r.at[n], (g, partner)).wait_recv()
    for r in range(4):
        a_piece(chip * 8 + 2 * r + core, ax_s.at[r], ax_r.at[r], (g, cross)).start()
    wo_cross(me).start()
    wo_partner(me).start()
    load_wo.start()

    for n in range(6):
        w_cross(n, me, wx).wait_recv()
        w_trade(n, wx).start()
    for copy in load_w:
        copy.wait()
    for m in range(3):
        w_partner(m, partner).wait_recv()
    for n in range(6):
        w_trade(n, wx_other).wait_recv()

    v_s[:, HEAD:, :] = jnp.ones((HEADS, SUMS, ROWS), jnp.bfloat16)

    def q_rows(n):
        return _rows(jnp.where(n // 4 == chip, n % 4, 4), CHUNK)

    def project(n):
        rows = _rows(n, CHUNK)
        cos, sin = [], []
        for s in range(2):
            near_cos, near_sin = near_ref[0], near_ref[1]
            far_cos, far_sin = far_ref[0, pl.ds(2 * n + s, 1), :], far_ref[1, pl.ds(2 * n + s, 1), :]
            cos.append(far_cos * near_cos - far_sin * near_sin)
            sin.append(far_sin * near_cos + far_cos * near_sin)
        cos, sin = jnp.concatenate(cos, 0), jnp.concatenate(sin, 0)
        for m, to in ((0, q_s), (1, k_s)):
            got = _dot(a_s[rows, :], w_s[m], 1, 0).astype(jnp.bfloat16).astype(jnp.float32)
            for h in range(HEADS):
                t = got[:, h * HEAD : (h + 1) * HEAD]
                to[h, q_rows(n) if m == 0 else rows, :] = (t * cos + pltpu.roll(t, HEAD // 2, 1) * sin).astype(jnp.bfloat16)
        got = _dot(a_s[rows, :], w_s[2], 1, 0)
        for h in range(HEADS):
            v_s[h, :HEAD, rows] = got[:, h * HEAD : (h + 1) * HEAD].T.astype(jnp.bfloat16)

    e = HEAD**-0.5 * LOG2E

    def attend(n):
        top_s[...] = jnp.full(top_s.shape, NEG, jnp.float32)
        mix_s[...] = jnp.zeros(mix_s.shape, jnp.float32)
        def block(j, masked):
            keys = _rows(j, CHUNK)
            scores = [_dot(k_s[h, keys, :], q_s[h, q_rows(n), :], 1, 1) for h in range(HEADS)]
            if masked:
                ok = lax.broadcasted_iota(jnp.int32, (CHUNK, CHUNK), 1) >= lax.broadcasted_iota(jnp.int32, (CHUNK, CHUNK), 0)
            weights, keeps = [], []
            for h, s in enumerate(scores):
                if masked:
                    s = jnp.where(ok, s, HIDDEN)
                old = top_s[h : h + 1, :]
                top = jnp.maximum(old, s.max(axis=0, keepdims=True))
                top_s[h : h + 1, :] = top
                weights.append(jnp.exp2((s - top) * e).astype(jnp.bfloat16))
                keeps.append(jnp.exp2((old - top) * e))
            for h in range(HEADS):
                mix_s[h] = mix_s[h] * keeps[h] + _dot(v_s[h, :, keys], weights[h], 1, 0)

        lax.fori_loop(0, n, lambda j, _: block(j, False), None)
        block(n, True)

    def results():
        each = []
        for h in range(HEADS):
            total = mix_s[h, HEAD : HEAD + 1, :]
            each.append((mix_s[h, :HEAD, :] * (1 / total)).T.astype(jnp.bfloat16))
        return jnp.concatenate(each, axis=1)

    def pass_wo_on():
        wo_cross(cross).wait_recv()
        wo_trade(g).start()
        wo_forward(cross, g, 0).start()

    lax.fori_loop(0, 4, lambda r, _: project(chip * 4 + r), None)

    def step(n, _):
        r, owner = n % 4, n // 2

        @pl.when(n // 4 != chip)
        def _():
            mine = far * 4 + 2 * r + core
            a_piece(mine, ax_s.at[r], ax_r.at[r], (g, cross)).wait_recv()
            a_piece(mine, af_s.at[r], af_r.at[r], (g, partner)).start()
            a_piece(far * 4 + 2 * r + 1 - core, af_s.at[r], af_r.at[r], (g, partner)).wait_recv()
            project(n)

        @pl.when((n == 6) & (chip == 1))
        def _():
            pass_wo_on()

        attend(n)

        @pl.when(owner == me)
        def _():
            seen_s[_rows(n % 2, CHUNK), _rows(me, WIDE)] = results()

        @pl.when(owner != me)
        def _():
            out_s[_rows(away(owner) * 2 + n % 2, CHUNK), :] = results()
            result(2 * n, me, owner).start()
            result(2 * n + 1, me, owner).start()

    lax.fori_loop(0, 8, step, None)

    for r in range(4):
        a_piece(me * 4 + r, ap_s.at[r], ap_r.at[r], (g, partner)).wait_send()
        a_piece(chip * 8 + 2 * r + core, ax_s.at[r], ax_r.at[r], (g, cross)).wait_send()
    for copy in again_x:
        copy.start()

    @pl.when(chip == 0)
    def _():
        pass_wo_on()

    wo_trade(1 - g).wait_recv()
    wo_forward(cross, 1 - g, 1).start()
    load_wo.wait()
    wo_partner(partner).wait_recv()
    for n in range(2):
        part = g if n == 0 else 1 - g
        wo_forward(far + 1 - core, part, n).wait_recv()
    for copy in again_x:
        copy.wait()

    def arrive(n, *others):
        for other in others:
            result(me * 4 + n, other, me).wait_recv()

    def product(n, j, start, depth):
        part = pl.ds(pl.multiple_of(start, OWN), depth)
        return _dot(seen_s[_rows(n, PIECE), part], wo_s[part, _rows(j, TILE)], 1, 0)

    def put(n, j, y):
        mine, at = _rows(me * 4 + n, PIECE), _rows(j, TILE)
        a_s[mine, at] = (a_s[mine, at].astype(jnp.float32) + y).astype(jnp.bfloat16)
        store(n, j).start()

    def whole(n, _):
        arrive(n, partner, cross, far + 1 - core)
        lax.fori_loop(0, D // TILE, lambda j, _: put(n, j, product(n, j, 0, D)), None)

    lax.fori_loop(0, 3, whole, None)

    arrive(3, partner)

    def near(j, _):
        part_s[:, _rows(j, TILE)] = product(3, j, chip * OWN, OWN)

    lax.fori_loop(0, D // TILE, near, None)
    arrive(3, cross, far + 1 - core)
    lax.fori_loop(0, D // TILE, lambda j, _: put(3, j, part_s[:, _rows(j, TILE)] + product(3, j, far * WIDE, OWN)), None)

    for n in range(6):
        w_cross(n, wx, me).wait_send()
        w_trade(n, wx).wait_send()
    for m in range(3):
        w_partner(m, me).wait_send()
    for r in range(4):
        a_piece(far * 4 + 2 * r + core, af_s.at[r], af_r.at[r], (g, partner)).wait_send()
    wo_cross(me).wait_send()
    wo_partner(me).wait_send()
    wo_trade(g).wait_send()
    wo_forward(cross, g, 0).wait_send()
    wo_forward(cross, 1 - g, 1).wait_send()

    def sent(n, _):
        @pl.when(n // 4 != me)
        def _():
            result(n, me, n // 4).wait_send()

    lax.fori_loop(0, 16, sent, None)
    for n in range(4):
        for j in range(D // TILE):
            store(n, j).wait()


def _take(here_ref, y_ref, held, load, store):
    part = OWN // held.shape[0]
    loads = [pltpu.make_async_copy(here_ref.at[pl.ds(n * part, part)], held.at[n], load.at[n]) for n in range(held.shape[0])]
    stores = [pltpu.make_async_copy(held.at[n], y_ref.at[pl.ds(n * part, part)], store.at[n]) for n in range(held.shape[0])]
    for copy in loads:
        copy.start()
    for got, put in zip(loads, stores):
        got.wait()
        put.start()
    for copy in stores:
        copy.wait()


def _turns(places):
    half = HEAD // 2
    angle = places[:, None].astype(np.float64) * THETA ** (-np.arange(half) / half)
    cos, sin = np.cos(angle), np.sin(angle)
    return np.stack([np.concatenate([cos, cos], 1), np.concatenate([-sin, sin], 1)]).astype(np.float32)


def solution(mesh):
    def step(x, gain, wq, wk, wv, wo):
        any_ = pl.BlockSpec(memory_space=pl.ANY)
        bf16, dma = jnp.bfloat16, pltpu.SemaphoreType.DMA
        here = pl.pallas_call(
            _kernel,
            out_shape=jax.ShapeDtypeStruct((OWN, D), bf16),
            in_specs=[any_] * 8,
            out_specs=any_,
            scratch_shapes=[
                pltpu.VMEM((D,), bf16),
                pltpu.VMEM((2, PIECE, HEAD), jnp.float32),
                pltpu.VMEM((2, ROWS // PIECE, HEAD), jnp.float32),
                pltpu.VMEM((ROWS, D), bf16),
                pltpu.VMEM((3, D, WIDE), bf16),
                pltpu.VMEM((D, D), bf16),
                pltpu.VMEM((HEADS, 5 * CHUNK, HEAD), bf16),
                pltpu.VMEM((HEADS, ROWS, HEAD), bf16),
                pltpu.VMEM((HEADS, HEAD + SUMS, ROWS), bf16),
                pltpu.VMEM((ROWS - OWN, WIDE), bf16),
                pltpu.VMEM((OWN, D), bf16),
                pltpu.VMEM((PIECE, D), jnp.float32),
                pltpu.VMEM((HEADS, CHUNK), jnp.float32),
                pltpu.VMEM((HEADS, HEAD + SUMS, CHUNK), jnp.float32),
                dma((15,)),
                dma((6,)), dma((6,)), dma((6,)), dma((6,)), dma((3,)), dma((3,)),
                dma((4,)), dma((4,)), dma((4,)), dma((4,)), dma((4,)), dma((4,)),
                dma, dma, dma, dma, dma, dma, dma((2,)), dma((2,)),
                dma((16,)), dma((4, 4)), dma((4, D // TILE)),
            ],
            compiler_params=pltpu.CompilerParams(collective_id=0, has_side_effects=True, vmem_limit_bytes=67043328),
        )(x, gain, wq, wk, wv, wo, jnp.asarray(_turns(np.arange(PIECE))), jnp.asarray(_turns(np.arange(ROWS // PIECE) * PIECE)))
        parts = 4
        return pl.pallas_call(
            _take,
            out_shape=jax.ShapeDtypeStruct((OWN, D), bf16),
            in_specs=[any_],
            out_specs=any_,
            scratch_shapes=[pltpu.VMEM((parts, OWN // parts, D), bf16), dma((parts,)), dma((parts,))],
        )(here)

    tokens, whole = P(("dp", "sp"), None), P("sp", None)
    return jax.shard_map(
        step,
        mesh=mesh,
        in_specs=(tokens, P(None), whole, whole, whole, whole),
        out_specs=tokens,
        check_vma=False,
    )
```
